32 devices in a mesh: row: 16 (over z, y, x), col: 2 (over core).
Axes of the slice: x: 2, y: 2, z: 4, core: 2. Of those that a mesh axis runs over, the one named last changes fastest.
Arguments:
- right_sides: bfloat16 [256, 128, 128], P('row'), may hold values from -6 to 6
- inverse_diag: bfloat16 [256, 128, 128], P('row'), may hold values from -0.5 to 0.5
- off_blocks: bfloat16 [2, 256, 6, 128, 128], P('col', 'row'), may hold values from -0.09375 to 0.09375
- owners: int32 [2, 256, 6], P('col', 'row'), may hold values from 0 to 15, all different within a row; in each aligned block of 16 rows (0 to 15, 16 to 31, ..., all dimensions but the last counted through in order) at most 8 rows name the same one
- local_block: int32 [2, 256, 6], P('col', 'row'), may hold values from 0 to 15
- counts: int32 [256], P('row'), may hold values from 6 to 12
Outputs:
- solved: bfloat16 [256, 128, 128], P('row')
The draws below stay inside these ranges and needn't reach their ends.
Inputs may be any that keep to these rules, and one draw needn't show every extreme that they name: In the 16 block rows of one device (aligned blocks of rows of the [2, 256] layout) a row's 6 entries are different owners, no owner is named more than 8 times, and in some blocks one owner exactly 8 times.
All inputs are finite; a program needn't handle non-finite values.
Results may differ from the reference program's by a relative error of at most 0.014.
Values may be sent and summed in bfloat16 or wider, within the bound.
No kernel may reach another device: no remote copies, remote signals or barrier semaphores. Data moves between devices by JAX's collectives and lax.ppermute only.
A program may use at most 64 MiB of HBM per device.

```python
import math
import jax
import jax.numpy as jnp
import numpy as np
from jax import lax

BLOCK = 128
RHS = 128
BR_DEV = 16
KD = 6
ITERS = 4
NB = 256
KSLOTS = 12
CAP = 8
N_ROW = 16
N_COL = 2


def set_ends(values, stream_key, smallest, top_value):
    extent = values.shape
    index_at = [jax.random.randint(jax.random.fold_in(stream_key, axis), (), 0, extent[axis]) for axis in range(len(extent))]
    values = values.at[tuple(index_at)].set(smallest)
    longest = extent.index(max(extent))
    index_at[longest] = (index_at[longest] + 1) % extent[longest]
    return values.at[tuple(index_at)].set(top_value)


def level_of(rng, dims, cuts, low, high):
    def one(position, shards_of):
        heights = jax.random.uniform(jax.random.fold_in(jax.random.fold_in(rng, 6), position), (shards_of,), jnp.float32, low / len(cuts), high / len(cuts))
        return jnp.repeat(jnp.exp(heights), dims[position] // shards_of).reshape((-1,) + (1,) * (len(dims) - position - 1))

    gain = one(*cuts[0])
    for cut in cuts[1:]:
        gain = gain * one(*cut)
    return gain


def routed_block(key, own, number, rows, count, top, limit, skew):
    ranking = jax.random.permutation(key, count)
    heavy_load, ordinary = load_shares(count, rows * top, limit, skew, True), load_shares(count, rows * top, limit, skew, False)
    places = jnp.arange(count)

    def named(lengths, turn):
        used = int((lengths > 0).sum())
        fixed = max(1, used // 4)
        passed = fixed + (places - fixed + turn * (used - fixed)) % max(1, count - fixed)
        return jnp.zeros((count,), jnp.int32).at[ranking[jnp.where(places < fixed, places, passed)]].set(jnp.asarray(lengths, jnp.int32))

    lengths = jnp.where(number % 4 == 0, named(heavy_load, number // 4), named(ordinary, number - number // 4 - 1))
    mixed = jax.random.permutation(jax.random.fold_in(own, 3), count)
    source_of, sink = mixed[0:count // 2 * 2:2], mixed[1:count // 2 * 2:2]
    margin = jnp.minimum(lengths[source_of] - 1, limit - lengths[sink]) // 2
    margin = jnp.where((source_of == ranking[0]) | (sink == ranking[0]) | (lengths[sink] == 0), 0, jnp.maximum(margin, 0))
    passed = jax.random.randint(jax.random.fold_in(own, 4), (count // 2,), 0, 1 << 20) % (margin + 1)
    lengths = lengths.at[source_of].add(-passed).at[sink].add(passed)
    labels = jnp.searchsorted(jnp.cumsum(lengths), jnp.arange(rows * top), side="right").astype(jnp.int32)
    table = labels.reshape(top, rows).T
    table = table[jax.random.permutation(jax.random.fold_in(own, 1), rows)]
    turn = jax.random.randint(jax.random.fold_in(own, 2), (rows, 1), 0, top)
    return jnp.take_along_axis(table, (jnp.arange(top)[None, :] + turn) % top, axis=1)


def load_shares(count, total, most, lean, full):
    loads = [(1 << 20) // math.isqrt(rank ** lean) + 1 for rank in range(1, count + 1)]
    largest = most if full else min(most, max(-(-total // count), total * loads[0] // sum(loads)))
    least = 1 if total - largest >= count - 1 else 0
    given, rest = [largest] + [least] * (count - 1), total - largest - least * (count - 1)
    while rest > 0:
        free = [i for i in range(1, count) if given[i] < largest] or [i for i in range(1, count) if given[i] < most]
        whole, left = sum([loads[i] for i in free]), rest
        for i in free:
            extra = min(most - given[i], max(1, left * loads[i] // whole), rest)
            given[i] = given[i] + extra
            rest = rest - extra
    return np.array(given)


def centred(key, dims, deviation, reach, shards=(), held_as=jnp.bfloat16):
    values = jax.random.normal(key, dims, jnp.float32) * deviation
    if len(shards) > 0:
        values = level_of(key, dims, shards, -0.22, 0.18) * values
    return jnp.clip(values, min=-reach, max=reach).astype(held_as)


def setup_inputs(seed: int = 0) -> dict:
    streams_of = jax.random.split(jax.random.key(seed), 7)
    right_sides = centred(streams_of[0], (NB, BLOCK, RHS), 1.0, 6.0, ((0, 16),))
    inverse_diag = centred(streams_of[1], (NB, BLOCK, BLOCK), BLOCK ** -0.5, 0.5, ((0, 16),))
    off_blocks = centred(streams_of[2], (N_COL, NB, KD, BLOCK, BLOCK), (3 * BLOCK * KSLOTS) ** -0.5, 0.09375, ((0, 2), (1, 16)))
    owners_keys = jax.random.split(jax.random.fold_in(streams_of[3], 1), N_COL * NB // BR_DEV)
    owners_turns = jax.random.permutation(jax.random.fold_in(streams_of[3], 3), N_COL * NB // BR_DEV)
    owners = jax.vmap(lambda own, number: routed_block(jax.random.fold_in(streams_of[3], 2), own, number, BR_DEV, N_ROW, KD, CAP, 2))(owners_keys, owners_turns).reshape((N_COL, NB, KD))
    local_block = set_ends(jax.random.randint(streams_of[4], (N_COL, NB, KD), 0, BR_DEV), jax.random.fold_in(streams_of[4], 1), 0, BR_DEV - 1).astype(jnp.int32)
    counts = set_ends(jax.random.randint(streams_of[5], (NB,), KSLOTS // 2, KSLOTS + 1), jax.random.fold_in(streams_of[5], 1), KSLOTS // 2, KSLOTS).astype(jnp.int32)
    return {"right_sides": right_sides, "inverse_diag": inverse_diag, "off_blocks": off_blocks, "owners": owners, "local_block": local_block, "counts": counts}


def apply_inverse(inverse, right):
    return jnp.einsum("bij,bjr->bir", inverse.astype(jnp.float32), right.astype(jnp.float32)).astype(jnp.bfloat16)


def reference(right_sides, inverse_diag, off_blocks, owners, local_block, counts):
    group_count = owners.shape[0]
    per_group = owners.shape[2]
    columns = (owners * BR_DEV + local_block).astype(jnp.int32)
    slot_index = jnp.arange(group_count, dtype=jnp.int32)[:, None, None] + group_count * jnp.arange(per_group, dtype=jnp.int32)[None, None, :]
    is_live = slot_index < counts[None, :, None]
    solved = apply_inverse(inverse_diag, right_sides)
    for iteration in range(ITERS - 1):
        current = solved

        def group_term(pieces):
            blocks, cols, live = pieces
            picked = current[cols].astype(jnp.float32)
            masked = jnp.where(live[:, :, None, None], blocks.astype(jnp.float32), jnp.zeros((), jnp.float32))
            return jnp.einsum("bkij,bkjr->bir", masked, picked).astype(jnp.bfloat16)

        partial_value = lax.map(group_term, (off_blocks, columns, is_live))
        off_sum = jnp.sum(partial_value.astype(jnp.float32), axis=0)
        corrected = (right_sides.astype(jnp.float32) - off_sum).astype(jnp.bfloat16)
        solved = apply_inverse(inverse_diag, corrected)
    return solved
```

```python
import jax
import jax.numpy as jnp
from jax import lax
from jax.experimental import pallas as pl
from jax.experimental.pallas import tpu as pltpu
from jax.sharding import PartitionSpec as P

ITERS = 4


NT = (((1,), (1,)), ((), ()))


def step_kernel(index_ref, *refs, mat_count, piece_count, piece_rows, width):
    mats = refs[:mat_count]
    right_ref, inverse_ref = refs[mat_count : mat_count + 2]
    pieces = refs[mat_count + 2 : mat_count + 2 + piece_count]
    out_ref, held, sems = refs[mat_count + 2 + piece_count :]
    row = pl.program_id(0)
    rows = pl.num_programs(0)

    @pl.when(row == 0)
    def _():
        copies = []
        start = 0
        for number, piece in enumerate(pieces):
            copies.append(
                pltpu.make_async_copy(
                    piece, held.at[pl.ds(start, piece_rows[number])], sems.at[number]
                )
            )
            start += piece_rows[number]
        for copy in copies:
            copy.start()
        held[pl.ds(start, width), :] = jnp.zeros((width, held.shape[1]), held.dtype)
        for copy in copies:
            copy.wait()

    off = None
    group = 0
    for mat in mats:
        per_group = mat.shape[2]
        for inner in range(mat.shape[0]):
            total = None
            for slot in range(per_group):
                place = index_ref[(group * rows + row) * per_group + slot]
                block = held[pl.ds(pl.multiple_of(place, width), width), :]
                term = lax.dot_general(
                    block, mat[inner, 0, slot], NT, preferred_element_type=jnp.float32
                )
                total = term if total is None else total + term
            total = total.astype(jnp.bfloat16).astype(jnp.float32)
            off = total if off is None else off + total
            group += 1
    corrected = (right_ref[0].astype(jnp.float32) - off).astype(jnp.bfloat16)
    out_ref[0] = lax.dot_general(
        corrected, inverse_ref[0], NT, preferred_element_type=jnp.float32
    ).astype(jnp.bfloat16)


def step(index, mats, right, inverse, pieces):
    rows, width, block = right.shape
    piece_rows = tuple(piece.shape[0] for piece in pieces)
    specs = [
        pl.BlockSpec((mat.shape[0], 1) + mat.shape[2:], lambda i, s: (0, i, 0, 0, 0))
        for mat in mats
    ]
    specs.append(pl.BlockSpec((1, width, block), lambda i, s: (i, 0, 0)))
    specs.append(pl.BlockSpec((1, block, block), lambda i, s: (i, 0, 0)))
    specs += [pl.BlockSpec(memory_space=pl.ANY)] * len(pieces)
    body = lambda *refs: step_kernel(
        *refs,
        mat_count=len(mats),
        piece_count=len(pieces),
        piece_rows=piece_rows,
        width=width,
    )
    return pl.pallas_call(
        body,
        out_shape=jax.ShapeDtypeStruct(right.shape, jnp.bfloat16),
        grid_spec=pltpu.PrefetchScalarGridSpec(
            num_scalar_prefetch=1,
            grid=(rows,),
            in_specs=specs,
            out_specs=pl.BlockSpec((1, width, block), lambda i, s: (i, 0, 0)),
            scratch_shapes=[
                pltpu.VMEM((sum(piece_rows) + width, block), jnp.bfloat16),
                pltpu.SemaphoreType.DMA((len(pieces),)),
            ],
        ),
        compiler_params=pltpu.CompilerParams(dimension_semantics=("arbitrary",)),
    )(index, *mats, right, inverse, *pieces)


def exchange(value, offsets, row_count):
    cores = len(offsets)
    pairs = [
        (r * cores + c, (r ^ offsets[c]) * cores + c)
        for r in range(row_count)
        for c in range(cores)
    ]
    return lax.ppermute(value, ("row", "col"), pairs)


def spread(own, row_count):
    one, two = (2, 1), (1, 2)
    layers = [(own, 0)]
    bit = row_count // 2
    while bit >= 4:
        layers += [(exchange(v, (bit, bit), row_count), o ^ bit) for v, o in layers]
        bit //= 2
    pieces, offsets = [], []
    for value, offset in layers:
        first = exchange(value, one, row_count)
        second = exchange(jnp.concatenate([value, first]), two, row_count)
        pieces += [value, first, second]
        offsets += [
            (offset, offset),
            (offset ^ one[0], offset ^ one[1]),
            (offset ^ two[0], offset ^ two[1]),
            (offset ^ 3, offset ^ 3),
        ]
    return pieces, offsets


def shards(right_sides, inverse_diag, off_blocks, owners, local_block, counts):
    row_count = lax.axis_size("row")
    col_count = lax.axis_size("col")
    row_index = lax.axis_index("row")
    col_index = lax.axis_index("col")
    rows, block, rhs = right_sides.shape
    per_group = owners.shape[2]
    width = rhs // col_count
    paired = col_count == 2 and row_count >= 4 and row_count & (row_count - 1) == 0

    global_slot = col_index + col_count * jnp.arange(per_group, dtype=jnp.int32)
    is_live = global_slot[None, :] < counts[:, None]
    wanted = jnp.where(is_live, owners[0] * rows + local_block[0], -1)
    if paired:
        other = [(c, 1 - c) for c in range(col_count)]
        mats = [off_blocks, lax.ppermute(off_blocks, "col", other)]
        wanted = jnp.stack([wanted, lax.ppermute(wanted, "col", other)])
    else:
        mats = [lax.all_gather(off_blocks, "col", axis=0, tiled=True)]
        wanted = lax.all_gather(wanted, "col", axis=0, tiled=False)

    right = jnp.swapaxes(right_sides, 1, 2)
    right = lax.dynamic_slice_in_dim(right, col_index * width, width, 1)
    solved = jnp.einsum(
        "bri,bmi->brm", right, inverse_diag, preferred_element_type=jnp.float32
    ).astype(jnp.bfloat16)

    index = None
    for iteration in range(ITERS - 1):
        own = solved.reshape(rows * width, block)
        if paired:
            pieces, offsets = spread(own, row_count)
        else:
            pieces = [lax.all_gather(own, "row", axis=0, tiled=True)]
        if index is None:
            owner = wanted // rows
            if paired:
                table = jnp.array(offsets, jnp.int32)[:, col_index]
                hit = (owner ^ row_index)[..., None] == table
                owner = jnp.sum(
                    jnp.where(hit, jnp.arange(row_count, dtype=jnp.int32), 0), axis=-1
                )
            place = (owner * rows + wanted % rows) * width
            index = jnp.where(wanted < 0, row_count * rows * width, place).reshape(-1)
        solved = step(index, mats, right, inverse_diag, pieces)

    if paired:
        theirs = lax.ppermute(solved, "col", other)
        mine_first = col_index == 0
        whole = jnp.concatenate(
            [jnp.where(mine_first, solved, theirs), jnp.where(mine_first, theirs, solved)], 1
        )
    else:
        whole = lax.all_gather(solved, "col", axis=1, tiled=True)
    return jnp.swapaxes(whole, 1, 2)


def solution(mesh):
    in_specs = (
        P("row", None, None),
        P("row", None, None),
        P("col", "row", None, None, None),
        P("col", "row", None),
        P("col", "row", None),
        P("row"),
    )
    out_specs = P("row", None, None)
    return jax.shard_map(shards, mesh=mesh, in_specs=in_specs, out_specs=out_specs, check_vma=False)
```

```python
import jax
import jax.numpy as jnp
from jax import lax
from jax.experimental import pallas as pl
from jax.experimental.pallas import tpu as pltpu
from jax.sharding import PartitionSpec as P


ITERS = 4
CHUNK = 4


NT = (((1,), (1,)), ((), ()))


def step_kernel(index_ref, *refs, mat_count, piece_count, piece_rows, width):
    mats = refs[:mat_count]
    right_ref, inverse_ref = refs[mat_count : mat_count + 2]
    pieces = refs[mat_count + 2 : mat_count + 2 + piece_count]
    out_ref, held, sems = refs[mat_count + 2 + piece_count :]
    row = pl.program_id(0)
    rows = pl.num_programs(0) * right_ref.shape[0]

    @pl.when(row == 0)
    def _():
        copies = []
        start = 0
        for number, piece in enumerate(pieces):
            copies.append(
                pltpu.make_async_copy(
                    piece, held.at[pl.ds(start, piece_rows[number])], sems.at[number]
                )
            )
            start += piece_rows[number]
        for copy in copies:
            copy.start()
        held[pl.ds(start, width), :] = jnp.zeros((width, held.shape[1]), held.dtype)
        for copy in copies:
            copy.wait()

    for local in range(right_ref.shape[0]):
        off = None
        group = 0
        for mat in mats:
            per_group = mat.shape[2]
            for inner in range(mat.shape[0]):
                blocks = []
                first = (group * rows + row * right_ref.shape[0] + local) * per_group
                for slot in range(per_group):
                    place = pl.multiple_of(index_ref[first + slot], width)
                    blocks.append(held[pl.ds(place, width), :])
                total = None
                for slot in range(per_group):
                    term = lax.dot_general(
                        blocks[slot],
                        mat[inner, local, slot],
                        NT,
                        preferred_element_type=jnp.float32,
                    )
                    total = term if total is None else total + term
                total = total.astype(jnp.bfloat16).astype(jnp.float32)
                off = total if off is None else off + total
                group += 1
        corrected = (right_ref[local].astype(jnp.float32) - off).astype(jnp.bfloat16)
        out_ref[local] = lax.dot_general(
            corrected, inverse_ref[local], NT, preferred_element_type=jnp.float32
        ).astype(jnp.bfloat16)


def step(index, mats, right, inverse, pieces):
    rows, width, block = right.shape
    chunk = CHUNK if rows % CHUNK == 0 else 1
    piece_rows = tuple(piece.shape[0] for piece in pieces)
    specs = [
        pl.BlockSpec((mat.shape[0], chunk) + mat.shape[2:], lambda i, s: (0, i, 0, 0, 0))
        for mat in mats
    ]
    specs.append(pl.BlockSpec((chunk, width, block), lambda i, s: (i, 0, 0)))
    specs.append(pl.BlockSpec((chunk, block, block), lambda i, s: (i, 0, 0)))
    specs += [pl.BlockSpec(memory_space=pl.ANY)] * len(pieces)
    body = lambda *refs: step_kernel(
        *refs,
        mat_count=len(mats),
        piece_count=len(pieces),
        piece_rows=piece_rows,
        width=width,
    )
    return pl.pallas_call(
        body,
        out_shape=jax.ShapeDtypeStruct(right.shape, jnp.bfloat16),
        grid_spec=pltpu.PrefetchScalarGridSpec(
            num_scalar_prefetch=1,
            grid=(rows // chunk,),
            in_specs=specs,
            out_specs=pl.BlockSpec((chunk, width, block), lambda i, s: (i, 0, 0)),
            scratch_shapes=[
                pltpu.VMEM((sum(piece_rows) + width, block), jnp.bfloat16),
                pltpu.SemaphoreType.DMA((len(pieces),)),
            ],
        ),
        compiler_params=pltpu.CompilerParams(dimension_semantics=("arbitrary",)),
    )(index, *mats, right, inverse, *pieces)


def exchange(value, offsets, row_count):
    cores = len(offsets)
    pairs = [
        (r * cores + c, (r ^ offsets[c]) * cores + c)
        for r in range(row_count)
        for c in range(cores)
    ]
    return lax.ppermute(value, ("row", "col"), pairs)


def spread(own, row_count):
    one, two = (2, 1), (1, 2)
    layers = [(own, 0)]
    bit = row_count // 2
    while bit >= 4:
        layers += [(exchange(v, (bit, bit), row_count), o ^ bit) for v, o in layers]
        bit //= 2
    pieces, offsets = [], []
    for value, offset in layers:
        first = exchange(value, one, row_count)
        both = jnp.concatenate([value, first])
        second = exchange(both, two, row_count)
        pieces += [value, first, second]
        offsets += [
            (offset, offset),
            (offset ^ one[0], offset ^ one[1]),
            (offset ^ two[0], offset ^ two[1]),
            (offset ^ 3, offset ^ 3),
        ]
    return pieces, offsets


def is_paired(row_count, col_count):
    return col_count == 2 and row_count >= 4 and row_count & (row_count - 1) == 0


def shards(right_sides, inverse_diag, off_blocks, owners, local_block, counts):
    row_count = lax.axis_size("row")
    col_count = lax.axis_size("col")
    row_index = lax.axis_index("row")
    col_index = lax.axis_index("col")
    rows, block, rhs = right_sides.shape
    per_group = owners.shape[2]
    width = rhs // col_count
    paired = is_paired(row_count, col_count)

    global_slot = col_index + col_count * jnp.arange(per_group, dtype=jnp.int32)
    is_live = global_slot[None, :] < counts[:, None]
    wanted = jnp.where(is_live, owners[0] * rows + local_block[0], -1)
    if paired:
        other = [(c, 1 - c) for c in range(col_count)]
        mats = [off_blocks, lax.ppermute(off_blocks, "col", other)]
        wanted = jnp.stack([wanted, lax.ppermute(wanted, "col", other)])
    else:
        mats = [lax.all_gather(off_blocks, "col", axis=0, tiled=True)]
        wanted = lax.all_gather(wanted, "col", axis=0, tiled=False)

    right = jnp.swapaxes(right_sides, 1, 2)
    right = lax.dynamic_slice_in_dim(right, col_index * width, width, 1)
    solved = jnp.einsum(
        "bri,bmi->brm", right, inverse_diag, preferred_element_type=jnp.float32
    ).astype(jnp.bfloat16)

    index = None
    for _ in range(ITERS - 1):
        own = solved.reshape(rows * width, block)
        if paired:
            pieces, offsets = spread(own, row_count)
        else:
            pieces = [lax.all_gather(own, "row", axis=0, tiled=True)]
        if index is None:
            owner = wanted // rows
            if paired:
                table = jnp.array(offsets, jnp.int32)[:, col_index]
                hit = (owner ^ row_index)[..., None] == table
                owner = jnp.sum(
                    jnp.where(hit, jnp.arange(row_count, dtype=jnp.int32), 0), axis=-1
                )
            place = (owner * rows + wanted % rows) * width
            index = jnp.where(wanted < 0, row_count * rows * width, place).reshape(-1)
        solved = step(index, mats, right, inverse_diag, pieces)

    if paired:
        theirs = lax.ppermute(solved, "col", other)
        mine_first = col_index == 0
        whole = jnp.concatenate(
            [jnp.where(mine_first, solved, theirs), jnp.where(mine_first, theirs, solved)], 1
        )
    else:
        whole = lax.all_gather(solved, "col", axis=1, tiled=True)
    return jnp.swapaxes(whole, 1, 2)


def solution(mesh):
    in_specs = (
        P("row", None, None),
        P("row", None, None),
        P("col", "row", None, None, None),
        P("col", "row", None),
        P("col", "row", None),
        P("row"),
    )
    out_specs = P("row", None, None)
    return jax.shard_map(
        shards, mesh=mesh, in_specs=in_specs, out_specs=out_specs, check_vma=False
    )
```
